32 devices in a mesh: dp: 4 (over x, core), fsdp: 4 (over z), mp: 2 (over y).
Axes of the slice: x: 2, y: 2, z: 4, core: 2. Of those that a mesh axis runs over, the one named last changes fastest.
Arguments:
- tokens_in: bfloat16 [4096, 3072], P(('dp', 'fsdp', 'mp')), may hold values from -40 to 40
- segment_ids: int32 [4096], P(('dp', 'fsdp', 'mp')), may hold values from 0 to 31, never falling along the last dimension, each value on 1 to 512 neighbouring positions
- target_ids: int32 [4096], P(('dp', 'fsdp', 'mp')), may hold values from 0 to 8191
- old_weights: bfloat16 [4, 3072, 2048], P(None, ('dp', 'fsdp', 'mp'))
- old_first: float32 [4, 3072, 2048], P(None, ('dp', 'fsdp', 'mp')), may hold values from -6 to 6
- old_second: float32 [4, 3072, 2048], P(None, ('dp', 'fsdp', 'mp')), may hold values from 0.01 to 4
- old_block: int32 [32], P(('dp', 'fsdp', 'mp')), may hold values from 0 to 31, each once
- new_residue: int32 [4], P('dp'), may hold values from 0 to 3, each once
- norm_gain: float32 [3072], replicated, may hold values from 0.5 to 1.5
- head_weight: bfloat16 [3072, 8192], P(None, ('fsdp', 'mp'))
Outputs:
- new_weights: bfloat16 [4, 3072, 2048], P(None, 'dp', ('fsdp', 'mp'))
- new_first: float32 [4, 3072, 2048], P(None, 'dp', ('fsdp', 'mp'))
- new_second: float32 [4, 3072, 2048], P(None, 'dp', ('fsdp', 'mp'))
- loss: float32 [4096], P(('dp', 'fsdp', 'mp'))
The draws below stay inside these ranges and needn't reach their ends.
Inputs may be any that keep to these rules, and one draw needn't show every extreme that they name: `old_block`: a permutation of the old layout's row blocks. `new_residue`: a permutation; index i of dp holds the rows whose number modulo 4 is new_residue[i], in rising order. `segment_ids`: never falling along the tokens.
All inputs are finite; a program needn't handle non-finite values.
Results may differ from the reference program's by a relative error of at most 0.0075.
Values may be sent and summed in bfloat16 or wider, within the bound.
A program may use at most 192 MiB of HBM per device.

```python
import math
import jax
import jax.numpy as jnp
import numpy as np
from jax import lax

D = 3072
HD = 128
HF = 2048
VOC = 8192
SEQ = 1024
TOKENS = 4096
N_DP = 4
N_FSDP = 4
N_MP = 2
DEVICES = 32


def draw_tokens_in(key, part):
    keys = jax.random.split(key, 1)
    drawn = jnp.clip(jax.random.normal(keys[0], (TOKENS, D), jnp.float32), -6.0, 6.0)
    return jnp.clip(drawn, -40.0, 40.0).astype(jnp.bfloat16)


def draw_old_weights(key, part):
    raw = jnp.clip(jax.random.normal(key, (4, D, HF), jnp.float32), -6.0, 6.0)
    fan_width = jnp.array([D, D, D, HF], jnp.float32).reshape(4, 1, 1)
    scaled = raw / jnp.sqrt(fan_width)
    return scaled.astype(jnp.bfloat16)


def draw_head_weight(key, part):
    keys = jax.random.split(key, 1)
    raw = jnp.clip(jax.random.normal(keys[0], (D, VOC), jnp.float32), -6.0, 6.0) / math.sqrt(D)
    return raw.astype(jnp.bfloat16)


def plant(result, own_key, least, largest):
    extent = result.shape
    index_at = [jax.random.randint(jax.random.fold_in(own_key, axis), (), 0, extent[axis]) for axis in range(len(extent))]
    result = result.at[tuple(index_at)].set(least)
    longest = extent.index(max(extent))
    index_at[longest] = (index_at[longest] + 1) % extent[longest]
    return result.at[tuple(index_at)].set(largest)


def levels(key, extent, cuts, low, top_value):
    def one(dim, shards_of):
        steps = jax.random.uniform(jax.random.fold_in(jax.random.fold_in(key, 6), dim), (shards_of,), jnp.float32, low / len(cuts), top_value / len(cuts))
        return jnp.repeat(jnp.exp(steps), extent[dim] // shards_of).reshape((-1,) + (1,) * (len(extent) - dim - 1))

    level = one(*cuts[0])
    for cut in cuts[1:]:
        level = level * one(*cut)
    return level


def rank_table(number_of, lean):
    loads = [(1 << 20) // math.isqrt(standing ** lean) + 1 for standing in range(1, number_of + 1)]
    deviation = 1 + sum(loads) // (1 << 30)
    return np.cumsum(np.array([max(1, weight // deviation) for weight in loads]))


def ranked(rng, dims, amount, slope):
    grid = rank_table(amount, slope)
    lot = jax.random.randint(jax.random.fold_in(rng, 1), dims, 0, int(grid[amount - 1]))
    grade = jnp.searchsorted(jnp.asarray(grid, jnp.int32), lot, side="right")
    return jax.random.permutation(jax.random.fold_in(rng, 2), amount)[grade].astype(jnp.int32)


def profile(number_of, total, bound, lean):
    loads = [(1 << 20) // math.isqrt(rank ** lean) + 1 for rank in range(2, number_of + 1)]
    spare, given = total - bound - (number_of - 1), [1] * (number_of - 1)
    while spare > 0:
        candidates = [i for i in range(number_of - 1) if given[i] < bound]
        pool, remaining = sum([loads[i] for i in candidates]), spare
        for i in candidates:
            addition = min(bound - given[i], max(1, remaining * loads[i] // pool), spare)
            given[i] = given[i] + addition
            spare = spare - addition
    return np.array([bound] + given)


def ragged(key, amount, total, reach, slope):
    if amount == 2:
        one = jax.random.randint(key, (), max(1, total - reach), min(reach, total - 1) + 1)
        return jnp.stack([one, total - one])
    lengths = jnp.asarray(profile(amount, total, reach, slope), jnp.int32)
    pairs = (amount - 1) // 2
    source_of, sink = lengths[1:1 + 2 * pairs:2], lengths[2:2 + 2 * pairs:2]
    margin = jnp.minimum(source_of - 1, reach - sink)
    moved = jax.random.randint(jax.random.fold_in(key, 1), (pairs,), 0, 1 << 20) % (margin + 1)
    lengths = lengths.at[1:1 + 2 * pairs:2].set(source_of - moved).at[2:2 + 2 * pairs:2].set(sink + moved)
    return lengths[jax.random.permutation(jax.random.fold_in(key, 2), amount)]


def centred(own_key, dims, spread, most, cuts=(), kind=jnp.bfloat16):
    values = jax.random.normal(own_key, dims, jnp.float32) * spread
    if len(cuts) > 0:
        values = levels(own_key, dims, cuts, -0.22, 0.18) * values
    return jnp.clip(values, min=-most, max=most).astype(kind)


def setup_inputs(seed: int = 0) -> dict:
    arg_keys = jax.random.split(jax.random.key(seed), 11)
    return {
        "tokens_in": draw_tokens_in(jax.random.fold_in(arg_keys[10], 71), 0),
        "segment_ids": jnp.searchsorted(jnp.cumsum(ragged(arg_keys[1], 8 * N_DP, TOKENS, SEQ // 2, 2)), jnp.arange(TOKENS), side="right").astype(jnp.int32),
        "target_ids": plant(ranked(arg_keys[2], (TOKENS,), VOC, 2), jax.random.fold_in(arg_keys[2], 3), 0, VOC - 1).astype(jnp.int32),
        "old_weights": draw_old_weights(jax.random.fold_in(arg_keys[10], 71), 0),
        "old_first": centred(arg_keys[4], (4, D, HF), 1.0, 6.0, ((1, 32),), jnp.float32),
        "old_second": jnp.clip(jnp.exp(math.log(4.0) - 5.9914646 * jax.random.uniform(arg_keys[5], (4, D, HF), jnp.float32) ** levels(arg_keys[5], (4, D, HF), ((1, 32),), -0.2, 0.2)), 0.01, 4.0),
        "old_block": jax.random.permutation(arg_keys[6], DEVICES).astype(jnp.int32),
        "new_residue": jax.random.permutation(arg_keys[7], N_DP).astype(jnp.int32),
        "norm_gain": jnp.clip(1.0 + 0.1 * jax.random.normal(arg_keys[8], (D,), jnp.float32), 0.5, 1.5),
        "head_weight": draw_head_weight(jax.random.fold_in(arg_keys[10], 71), 0),
    }


def inverse_table(table):
    total_count = table.shape[0]
    return jnp.zeros((total_count,), jnp.int32).at[table].set(jnp.arange(total_count, dtype=jnp.int32))

def logical_rows(stored, holder):
    matrices, row_count, columns = stored.shape
    devices = holder.shape[0]
    split_rows = stored.reshape(matrices, devices, row_count // devices, columns)
    return jnp.take(split_rows, holder, axis=1).reshape(matrices, row_count, columns)

def new_layout(logical, new_residue):
    matrices, row_count, columns = logical.shape
    dp_count = new_residue.shape[0]
    picked = jnp.take(logical.reshape(matrices, row_count // dp_count, dp_count, columns), new_residue, axis=2)
    return picked.transpose(0, 2, 1, 3).reshape(matrices, row_count, columns)

def one_sequence(tokens, segments, targets, weights, norm_gain, head_weight):
    seq_len = tokens.shape[0]
    columns = weights.shape[2]
    heads = columns // HD
    groups = N_FSDP * N_MP
    group_cols = columns // groups
    queries = jnp.dot(tokens, weights[0], preferred_element_type=jnp.float32).astype(jnp.bfloat16)
    keys_all = jnp.dot(tokens, weights[1], preferred_element_type=jnp.float32).astype(jnp.bfloat16)
    values_all = jnp.dot(tokens, weights[2], preferred_element_type=jnp.float32).astype(jnp.bfloat16)
    queries = queries.reshape(seq_len, heads, HD).astype(jnp.float32)
    keys_all = keys_all.reshape(seq_len, heads, HD).astype(jnp.float32)
    values_all = values_all.reshape(seq_len, heads, HD).astype(jnp.float32)
    positions = jnp.arange(seq_len, dtype=jnp.int32)
    allowed = (positions[:, None] >= positions[None, :]) & (segments[:, None] == segments[None, :])
    scores = jnp.einsum('shd,thd->hst', queries, keys_all) * (1.0 / math.sqrt(HD))
    scores = jnp.where(allowed[None], scores, -1e+30)
    row_max = lax.optimization_barrier(jnp.max(scores, axis=2, keepdims=True))
    expo = jnp.where(allowed[None], jnp.exp(scores - row_max), 0.0)
    soft = (expo / lax.optimization_barrier(jnp.sum(expo, axis=2, keepdims=True))).astype(jnp.bfloat16)
    attended = jnp.einsum('hst,thd->shd', soft.astype(jnp.float32), values_all).astype(jnp.bfloat16)
    attended = attended.reshape(seq_len, groups, group_cols).astype(jnp.float32)
    out_proj = weights[3].reshape(-1, groups, group_cols).astype(jnp.float32)
    parts = jnp.einsum('sgc,dgc->gsd', attended, out_proj).astype(jnp.bfloat16)
    parts = lax.optimization_barrier(parts)
    summed = lax.optimization_barrier(jnp.sum(parts.astype(jnp.float32), axis=0))
    hidden = tokens.astype(jnp.float32) + summed
    scale = lax.rsqrt(lax.optimization_barrier(jnp.mean(hidden * hidden, axis=1, keepdims=True)) + 1e-05)
    normed = (hidden * scale * norm_gain).astype(jnp.bfloat16)
    logits = jnp.dot(normed, head_weight, preferred_element_type=jnp.float32)
    row_top = lax.optimization_barrier(jnp.max(logits, axis=1))
    row_total = lax.optimization_barrier(jnp.sum(jnp.exp(logits - row_top[:, None]), axis=1))
    vocab_ids = jnp.arange(logits.shape[1], dtype=jnp.int32)
    picked = lax.optimization_barrier(jnp.sum(jnp.where(vocab_ids[None, :] == targets[:, None], logits, 0.0), axis=1))
    return row_top + jnp.log(row_total) - picked

def reference(tokens_in, segment_ids, target_ids, old_weights, old_first, old_second, old_block, new_residue, norm_gain, head_weight):
    holder = inverse_table(old_block)
    weights = logical_rows(old_weights, holder)
    new_weights = new_layout(weights, new_residue)
    new_first = new_layout(logical_rows(old_first, holder), new_residue)
    new_second = new_layout(logical_rows(old_second, holder), new_residue)
    seq_tokens = tokens_in.reshape(N_DP, SEQ, D)
    seq_segments = segment_ids.reshape(N_DP, SEQ)
    seq_targets = target_ids.reshape(N_DP, SEQ)

    def per_sequence(packed):
        return one_sequence(packed[0], packed[1], packed[2], weights, norm_gain, head_weight)
    losses = lax.map(per_sequence, (seq_tokens, seq_segments, seq_targets))
    return (new_weights, new_first, new_second, losses.reshape(TOKENS))
```

```python
import math

import jax
import jax.numpy as jnp
from jax import lax
from jax.sharding import PartitionSpec as P

HD = 128


def inverse_of(table):
    total_count = table.shape[0]
    places = jnp.arange(total_count, dtype=jnp.int32)
    return jnp.sum(jnp.where(table[None, :] == places[:, None], places[None, :], 0), axis=1)


def pack_rows(stored, residues, fm_count):
    matrices, row_count, columns = stored.shape
    dp_count = residues.shape[0]
    split_rows = stored.reshape(
        matrices, row_count // dp_count, dp_count, fm_count, columns // fm_count
    )
    chosen = jnp.take(split_rows, residues, axis=2, mode="clip")
    return chosen.transpose(2, 3, 0, 1, 4).reshape(
        dp_count * fm_count, matrices, row_count // dp_count, columns // fm_count
    )


def unpack_rows(received, holder):
    ordered = jnp.take(received, holder, axis=0, mode="clip")
    devices, matrices, pair_rows, group_cols = ordered.shape
    return ordered.transpose(1, 0, 2, 3).reshape(matrices, devices * pair_rows, group_cols)


def norm_rows(hidden, norm_gain):
    scale = lax.rsqrt(jnp.mean(hidden * hidden, axis=1, keepdims=True) + 1e-05)
    return (hidden * scale * norm_gain).astype(jnp.bfloat16)


FLAGS = dict(tail="a2a", first="before_rs", second="free", tokens="first")


def share_tables(segment_ids, target_ids, old_block, new_residue):
    axes = ("dp", "fsdp", "mp")
    own = jnp.concatenate([segment_ids, target_ids, old_block, new_residue])
    rows = jnp.broadcast_to(own[None, None], (lax.axis_size(axes), 1, own.shape[0]))
    rows = lax.all_to_all(rows, axes, split_axis=0, concat_axis=0, tiled=True)[:, 0]
    count = segment_ids.shape[0]
    fm_count = lax.axis_size(("fsdp", "mp"))
    here = lax.dynamic_slice_in_dim(rows, lax.axis_index("dp") * fm_count, fm_count)
    segments = here[:, :count].reshape(-1)
    targets = here[:, count : 2 * count].reshape(-1)
    return segments, targets, rows[:, 2 * count], rows[::fm_count, 2 * count + 1]


def joint_loss(row_top, row_total, picked):
    axes = ("fsdp", "mp")
    fm_count = lax.axis_size(axes)
    parts = jnp.stack([row_top, row_total, picked])
    own_count = parts.shape[1] // fm_count
    if FLAGS["tail"] == "a2a":
        parts = parts.reshape(3, fm_count, own_count).transpose(1, 0, 2)
        parts = lax.all_to_all(parts, axes, split_axis=0, concat_axis=0, tiled=True)
    else:
        place = lax.axis_index(axes)
        rows = jnp.zeros((fm_count,) + parts.shape, jnp.float32)
        rows = lax.psum(lax.dynamic_update_slice(rows, parts[None], (place, 0, 0)), axes)
        parts = lax.dynamic_slice_in_dim(rows, place * own_count, own_count, axis=2)
    tops, totals, targets = parts[:, 0], parts[:, 1], parts[:, 2]
    joint_max = jnp.max(tops, axis=0)
    joint_total = jnp.sum(totals * jnp.exp(tops - joint_max[None]), axis=0)
    return joint_max + jnp.log(joint_total) - jnp.sum(targets, axis=0)


def body(
    tokens_in,
    segment_ids,
    target_ids,
    old_weights,
    old_first,
    old_second,
    old_block,
    new_residue,
    norm_gain,
    head_weight,
):
    dp_count = lax.axis_size("dp")
    fm_count = lax.axis_size(("fsdp", "mp"))
    everyone = ("dp", "fsdp", "mp")
    columns = old_weights.shape[2]
    group_cols = columns // fm_count
    model_width = tokens_in.shape[1]
    new_rows = model_width // dp_count
    segments, targets, table_all, residues = share_tables(
        segment_ids, target_ids, old_block, new_residue
    )
    holder = inverse_of(table_all)
    inverse_res = inverse_of(residues)
    feature_ids = (
        residues[:, None] + dp_count * jnp.arange(new_rows, dtype=jnp.int32)[None]
    ).reshape(-1)
    logical_ids = (
        jnp.arange(new_rows, dtype=jnp.int32)[:, None] + new_rows * inverse_res[None]
    ).reshape(-1)
    own_picked = jnp.take(tokens_in, feature_ids, axis=1, mode="clip")
    picked_cols = lax.all_gather(own_picked, ("fsdp", "mp"), axis=0, tiled=True)
    seq_len = picked_cols.shape[0]
    weights_sent = pack_rows(old_weights, residues, fm_count)
    weights_got = lax.all_to_all(
        weights_sent, everyone, split_axis=0, concat_axis=0, tiled=True
    )
    first_sent = pack_rows(old_first, residues, fm_count)
    second_sent = pack_rows(old_second, residues, fm_count)
    if FLAGS["first"] != "free":
        weights_got, first_sent, second_sent = lax.optimization_barrier(
            (weights_got, first_sent, second_sent)
        )
    new_weights = unpack_rows(weights_got, holder)
    projections = new_weights[:3]
    if FLAGS.get("tokens") == "first":
        picked_cols, projections, first_sent = lax.optimization_barrier(
            (picked_cols, projections, first_sent)
        )
    first_got = lax.all_to_all(first_sent, everyone, split_axis=0, concat_axis=0, tiled=True)
    piece = lax.all_gather(projections, "dp", axis=1, tiled=True)
    projected = jnp.einsum("sr,mrc->msc", picked_cols, piece, preferred_element_type=jnp.float32)
    heads = group_cols // HD
    queries = projected[0].astype(jnp.bfloat16).reshape(seq_len, heads, HD)
    keys_all = projected[1].astype(jnp.bfloat16).reshape(seq_len, heads, HD)
    values_all = projected[2].astype(jnp.bfloat16).reshape(seq_len, heads, HD)
    positions_all = jnp.arange(seq_len, dtype=jnp.int32)
    allowed = (positions_all[:, None] >= positions_all[None, :]) & (
        segments[:, None] == segments[None, :]
    )
    scores = jnp.einsum("shd,thd->hst", queries, keys_all, preferred_element_type=jnp.float32) * (
        1.0 / math.sqrt(HD)
    )
    scores = jnp.where(allowed[None], scores, -1e30)
    row_max = jnp.max(scores, axis=2, keepdims=True)
    expo = jnp.where(allowed[None], jnp.exp(scores - row_max), 0.0)
    soft = (expo / jnp.sum(expo, axis=2, keepdims=True)).astype(jnp.bfloat16)
    attended = jnp.einsum("hst,thd->shd", soft, values_all, preferred_element_type=jnp.float32)
    attended = attended.astype(jnp.bfloat16).reshape(seq_len, group_cols)
    shuffled = jnp.einsum(
        "sc,rc->sr",
        attended,
        lax.all_gather(new_weights[3], "dp", axis=0, tiled=True),
        preferred_element_type=jnp.float32,
    )
    partial_value = shuffled.astype(jnp.bfloat16)
    if FLAGS["first"] == "rs_first":
        partial_value, second_sent = lax.optimization_barrier((partial_value, second_sent))
    if FLAGS["first"] == "before_rs":
        partial_value, first_got, second_sent = lax.optimization_barrier(
            (partial_value, first_got, second_sent)
        )
    second_got = lax.all_to_all(second_sent, everyone, split_axis=0, concat_axis=0, tiled=True)
    own_sum = lax.psum_scatter(
        partial_value, ("fsdp", "mp"), scatter_dimension=0, tiled=True
    )
    own_sum = jnp.take(own_sum, logical_ids, axis=1, mode="clip").astype(jnp.float32)
    own_normed = norm_rows(tokens_in.astype(jnp.float32) + own_sum, norm_gain)
    if FLAGS["second"] == "before_ag":
        own_normed, second_got = lax.optimization_barrier((own_normed, second_got))
    new_first = unpack_rows(first_got, holder)
    new_second = unpack_rows(second_got, holder)
    normed = lax.all_gather(own_normed, ("fsdp", "mp"), axis=0, tiled=True)
    logits = jnp.dot(normed, head_weight, preferred_element_type=jnp.float32)
    vocab_dev = logits.shape[1]
    offset = lax.axis_index(("fsdp", "mp")) * vocab_dev
    row_top = jnp.max(logits, axis=1)
    row_total = jnp.sum(jnp.exp(logits - row_top[:, None]), axis=1)
    vocab_ids = jnp.arange(vocab_dev, dtype=jnp.int32) + offset
    picked = jnp.sum(jnp.where(vocab_ids[None, :] == targets[:, None], logits, 0.0), axis=1)
    loss = joint_loss(row_top, row_total, picked)
    return (new_weights, new_first, new_second, loss)


def solution(mesh):
    placed = (
        P(("dp", "fsdp", "mp"), None),
        P(("dp", "fsdp", "mp")),
        P(("dp", "fsdp", "mp")),
        P(None, ("dp", "fsdp", "mp"), None),
        P(None, ("dp", "fsdp", "mp"), None),
        P(None, ("dp", "fsdp", "mp"), None),
        P(("dp", "fsdp", "mp")),
        P("dp"),
        P(),
        P(None, ("fsdp", "mp")),
    )
    return jax.shard_map(
        body,
        mesh=mesh,
        in_specs=placed,
        out_specs=(
            P(None, "dp", ("fsdp", "mp")),
            P(None, "dp", ("fsdp", "mp")),
            P(None, "dp", ("fsdp", "mp")),
            P(("dp", "fsdp", "mp")),
        ),
        check_vma=False,
    )
```
